768 devices in a mesh: section: 24 (over z, x_lo), dp: 4 (over x_hi, core), mp: 8 (over y).
Axes of the slice: x: 4 (x_hi: 2, x_lo: 2; x = x_hi * 2 + x_lo), y: 8, z: 12, core: 2. Of those that a mesh axis runs over, the one named last changes fastest.
Arguments:
- section_in: bfloat16 [2, 24, 256, 12288], P(None, 'section', 'dp'), may hold values from -6 to 6
- out_grad: bfloat16 [2, 24, 256, 12288], P(None, 'section', 'dp'), may hold values from -1.5 to 1.5
- lengths: int32 [2, 24, 4], P(None, 'section', 'dp'), may hold values from 1 to 64, as said below
- w_in: bfloat16 [24, 2, 192, 128, 128], P('section', None, 'mp'), as said below
- w_out: bfloat16 [24, 2, 192, 128, 128], P('section', None, 'mp'), as said below
- idx_in: int32 [24, 2, 192], P('section', None, 'mp'), may hold values from 0 to 95, as said below
- idx_out: int32 [24, 2, 192], P('section', None, 'mp'), may hold values from 0 to 95, as said below
Outputs:
- passed: bfloat16 [2, 24, 256, 12288], P(None, 'section', ('dp', 'mp'))
- grads: float32 [24, 2, 8, 24, 128, 128], P(None, None, 'mp', 'section', 'dp')
The draws below stay inside these ranges and needn't reach their ends.
Inputs may be any that keep to these rules, and one draw needn't show every extreme that they name: `lengths`: some micro-batch is full and some has a single live row. w_in[s, 1] equals w_in[23 - s, 0]: copy 1 at section s is the up relay's replica of layer 23 - s. w_out[s, 1] equals w_out[23 - s, 0]. idx_in[s, 1] equals idx_in[23 - s, 0]. idx_out[s, 1] equals idx_out[23 - s, 0].
All inputs are finite; a program needn't handle non-finite values.
Results may differ from the reference program's by a relative error of at most 0.0095.
Values may be sent and summed in bfloat16 or wider, within the bound.
A program may use at most 64 MiB of HBM per device.

```python
import math
import jax
import jax.numpy as jnp
from jax import lax

D = 12288
BLK = 128
MB = 64
SECTIONS = 24
REPLICAS = 4
TOKENS = 256
FBT = 192
FB_DEV = 24
N_MP = 8


def draw_w_in(key, part):
    inner = jax.random.fold_in(key, 11)
    base = jax.random.normal(inner, (SECTIONS, FBT, BLK, BLK), jnp.float32)
    base = base * (1.0 / math.sqrt(BLK))
    return jnp.stack([base, jnp.flip(base, 0)], axis=1).astype(jnp.bfloat16)


def draw_w_out(key, part):
    inner = jax.random.fold_in(key, 12)
    base = jax.random.normal(inner, (SECTIONS, FBT, BLK, BLK), jnp.float32)
    base = base * (1.0 / math.sqrt(BLK * max(1, FBT // (D // BLK))))
    return jnp.stack([base, jnp.flip(base, 0)], axis=1).astype(jnp.bfloat16)


def draw_idx_in(key, part):
    base = jax.random.randint(jax.random.fold_in(key, 13), (SECTIONS, FBT), 0, D // BLK, jnp.int32)
    return jnp.stack([base, jnp.flip(base, 0)], axis=1)


def draw_idx_out(key, part):
    base = jax.random.randint(jax.random.fold_in(key, 14), (SECTIONS, FBT), 0, D // BLK, jnp.int32)
    return jnp.stack([base, jnp.flip(base, 0)], axis=1)


def draw_lengths(key, part):
    drawn = jax.random.randint(jax.random.fold_in(key, 15), (2, SECTIONS, REPLICAS), 1, MB + 1, jnp.int32)
    return drawn.at[0, 0, 0].set(MB).at[1, -1, -1].set(1)


def shard_levels(own_key, dims, split, smallest, largest):
    def one(axis_at, shards_of):
        steps = jax.random.uniform(jax.random.fold_in(jax.random.fold_in(own_key, 6), axis_at), (shards_of,), jnp.float32, smallest / len(split), largest / len(split))
        return jnp.repeat(jnp.exp(steps), dims[axis_at] // shards_of).reshape((-1,) + (1,) * (len(dims) - axis_at - 1))

    factor_of = one(*split[0])
    for cut in split[1:]:
        factor_of = factor_of * one(*cut)
    return factor_of


def normal_values(stream_key, shape, width, bound, pieces=(), kind=jnp.bfloat16):
    level = shard_levels(stream_key, shape, pieces, -0.22, 0.18) if pieces else 1.0
    values = jax.random.normal(stream_key, shape, jnp.float32) * width * level
    return jnp.minimum(jnp.maximum(values, -bound), bound).astype(kind)


def setup_inputs(seed: int = 0) -> dict:
    keys = jax.random.split(jax.random.key(seed), 8)
    section_in = normal_values(keys[0], (2, SECTIONS, TOKENS, D), 1.0, 6.0, ((1, 24), (2, 4)))
    out_grad = normal_values(keys[1], (2, SECTIONS, TOKENS, D), 0.25, 1.5, ((1, 24), (2, 4)))
    lengths = draw_lengths(jax.random.fold_in(keys[7], 71), 0)
    w_in = draw_w_in(jax.random.fold_in(keys[7], 71), 0)
    w_out = draw_w_out(jax.random.fold_in(keys[7], 71), 0)
    idx_in = draw_idx_in(jax.random.fold_in(keys[7], 71), 0)
    idx_out = draw_idx_out(jax.random.fold_in(keys[7], 71), 0)
    return {"section_in": section_in, "out_grad": out_grad, "lengths": lengths, "w_in": w_in, "w_out": w_out, "idx_in": idx_in, "idx_out": idx_out}


def gelu_back(pre, upstream):
    return jax.vjp(lambda value: jax.nn.gelu(value, approximate=True), pre)[1](upstream)[0]

def section_pass(operands):
    inputs, masked, weight_in, weight_out, index_in, index_out = operands
    count = D // BLK
    in_blocks = inputs.reshape(TOKENS, count, BLK)
    back_blocks = masked.reshape(TOKENS, count, BLK)
    picked = jnp.take(in_blocks, index_in, axis=1)
    back = jnp.take(back_blocks, index_out, axis=1)
    pre = jnp.einsum('tjc,jcd->tjd', picked.astype(jnp.float32), weight_in.astype(jnp.float32))
    act = jax.nn.gelu(pre, approximate=True).astype(jnp.bfloat16)
    back_pre = jnp.einsum('tjd,jcd->tjc', back.astype(jnp.float32), weight_out.astype(jnp.float32))
    grad_pre = gelu_back(pre, back_pre).astype(jnp.bfloat16)
    terms = jnp.einsum('tjd,jcd->tjc', grad_pre.astype(jnp.float32), weight_in.astype(jnp.float32))
    terms = terms.reshape(TOKENS, N_MP, FB_DEV, BLK)
    onehot = jax.nn.one_hot(index_in.reshape(N_MP, FB_DEV), count, dtype=jnp.float32)
    share = jnp.einsum('tmjc,mjb->tmbc', terms, onehot, precision=lax.Precision.HIGHEST).astype(jnp.bfloat16)
    summed = lax.optimization_barrier(jnp.sum(share.astype(jnp.float32), axis=1)).reshape(TOKENS, D)
    grad_x = (masked.astype(jnp.float32) + summed).astype(jnp.bfloat16)
    picked_r = picked.astype(jnp.float32).reshape(REPLICAS, MB, FBT, BLK)
    grad_r = grad_pre.astype(jnp.float32).reshape(REPLICAS, MB, FBT, BLK)
    act_r = act.astype(jnp.float32).reshape(REPLICAS, MB, FBT, BLK)
    back_r = back.astype(jnp.float32).reshape(REPLICAS, MB, FBT, BLK)
    part_in = jnp.einsum('rtjc,rtjd->rjcd', picked_r, grad_r).astype(jnp.bfloat16)
    part_out = jnp.einsum('rtjc,rtjd->rjcd', act_r, back_r).astype(jnp.bfloat16)
    grad_in = lax.optimization_barrier(jnp.sum(part_in.astype(jnp.float32), axis=0))
    grad_out = lax.optimization_barrier(jnp.sum(part_out.astype(jnp.float32), axis=0))
    return (grad_x, grad_in, grad_out)

def reference(section_in, out_grad, lengths, w_in, w_out, idx_in, idx_out):
    positions = jnp.arange(MB, dtype=jnp.int32)
    live = (positions[None, None, None, :] < lengths[:, :, :, None]).reshape(2, SECTIONS, TOKENS)
    masked = jnp.where(live[:, :, :, None], out_grad, jnp.zeros((), out_grad.dtype))
    results = []
    for pipe in range(2):
        results.append(lax.map(section_pass, (section_in[pipe], masked[pipe], w_in[:, pipe], w_out[:, pipe], idx_in[:, pipe], idx_out[:, pipe])))
    down_dx, down_in, down_out = results[0]
    up_dx, up_in, up_out = results[1]
    empty = jnp.zeros((1, TOKENS, D), down_dx.dtype)
    from_next = jnp.concatenate([down_dx[1:], empty], axis=0)
    from_prev = jnp.concatenate([empty, up_dx[:-1]], axis=0)
    passed = jnp.stack([from_next, from_prev], axis=0)
    total_in = down_in + jnp.flip(up_in, 0)
    total_out = down_out + jnp.flip(up_out, 0)
    grads = jnp.stack([total_in, total_out], axis=1).reshape(SECTIONS, 2, N_MP, FB_DEV, BLK, BLK)
    return (passed, grads)
```

```python
import functools

import jax
import jax.numpy as jnp
from jax import lax
from jax.experimental import pallas as pl
from jax.experimental.pallas import tpu as pltpu
from jax.sharding import PartitionSpec as P

MESH = pl.DeviceIdType.MESH
F32 = jnp.float32
BF16 = jnp.bfloat16
ROOT = 0.7978845608028654
CUBIC = 0.044715


def contract(a, b, da, db):
    return lax.dot_general(a, b, (((da,), (db,)), ((), ())), preferred_element_type=F32)


def kernel(
    nz, nmp,
    len_ref, ii_ref, io_ref, x_hbm, g_hbm, wi_hbm, wo_hbm,
    passed_ref, grads_ref,
    x0, x1, g0, g1, wiv, wov, part, from_core, pair, from_x, ready, landed,
    terms, got, code, codes, dx, dx_in,
    in_sem, a_send, a_recv, b_send, b_recv, c_send, c_recv,
    t_send, t_recv, k_send, k_recv, d_send, d_recv,
):
    ns = 2 * nz
    s = lax.axis_index("section")
    r = lax.axis_index("dp")
    m = lax.axis_index("mp")
    z, xl = s // 2, lax.rem(s, 2)
    xh, c = r // 2, lax.rem(r, 2)
    rows, width = x0.shape
    count = width // 128
    xs, gs = (x0, x1), (g0, g1)

    def dev(section, dp, mp):
        return {"section": section, "dp": dp, "mp": mp}

    partner = dev(s, 2 * xh + (1 - c), m)
    across = dev(s, 2 * (1 - xh) + c, m)
    sides = [dev(2 * z + (1 - xl), 2 * h + c, m) for h in range(2)]
    down = dev(lax.rem(s + ns - 1, ns), r, m)
    up = dev(lax.rem(s + 1, ns), r, m)

    def along_z(k):
        half = (k + 1) // 2
        to = jnp.where(lax.rem(k, 2) == 0, z + (nz // 2 - k // 2), z - (nz // 2 - half))
        return lax.rem(to + nz, nz)

    def along_y(k):
        half = (k + 1) // 2
        to = jnp.where(lax.rem(k, 2) == 0, m + (nmp // 2 - k // 2), m - (nmp // 2 - half))
        return lax.rem(to + nmp, nmp)

    barrier = pltpu.get_barrier_semaphore()

    def greet(target):
        pl.semaphore_signal(barrier, inc=1, device_id=target, device_id_type=MESH)

    for target in [partner, across, sides[0], sides[1], down, up]:
        greet(target)

    @pl.loop(0, nz - 1)
    def _(k):
        greet(dev(2 * along_z(k) + xl, r, m))

    @pl.loop(0, nmp - 1)
    def _(k):
        greet(dev(s, r, along_y(k)))

    loads = []
    for p in range(2):
        loads.append([
            pltpu.make_async_copy(x_hbm.at[p], xs[p], in_sem.at[p, 0]),
            pltpu.make_async_copy(wi_hbm.at[p], wiv.at[p], in_sem.at[p, 1]),
            pltpu.make_async_copy(g_hbm.at[p], gs[p], in_sem.at[p, 2]),
            pltpu.make_async_copy(wo_hbm.at[p], wov.at[p], in_sem.at[p, 3]),
        ])
        for load in loads[p]:
            load.start()

    wide = code.shape[1]
    lane = lax.broadcasted_iota(jnp.int32, (8, wide), 1)
    relay = lax.broadcasted_iota(jnp.int32, (8, wide), 0)
    value = jnp.full((8, wide), -1, jnp.int32)
    for j in range(2 * nz):
        chosen = jnp.where(relay == 0, ii_ref[0, j], ii_ref[1, j])
        value = jnp.where(lane // 8 == j, chosen * 8 + lane % 8, value)
    code[...] = value

    def compute(p):
        live = lax.broadcasted_iota(jnp.int32, (rows, 128), 0) < len_ref[p]

        @pl.loop(0, nz)
        def _(q):
            kept = []
            for u in range(2):
                j = 2 * q + u
                at_in = ii_ref[p, j] * 128
                at_out = io_ref[p, j] * 128
                x = xs[p][:, pl.ds(at_in, 128)]
                back = jnp.where(live, gs[p][:, pl.ds(at_out, 128)].astype(F32), 0.0).astype(BF16)
                wi = wiv[p, j]
                wo = wov[p, j]
                pre = contract(x, wi, 1, 0)
                back_pre = contract(back, wo, 1, 1)
                square = pre * pre
                t = jnp.tanh(ROOT * (pre + CUBIC * (square * pre)))
                half = 0.5 * (1.0 + t)
                act = (pre * half).astype(BF16)
                slope = half + (0.5 * pre) * (1.0 - t * t) * (ROOT * (1.0 + (3.0 * CUBIC) * square))
                grad = (back_pre * slope).astype(BF16)
                kept.append(contract(grad, wi, 1, 1))
                g_in = contract(x, grad, 0, 0).astype(BF16)
                g_out = contract(act, back, 0, 0).astype(BF16)
                for h in range(2):
                    for d in range(2):
                        lo = 32 * (2 * h + d)
                        part[2 * p, d, u, h, q] = g_in[lo:lo + 32]
                        part[2 * p + 1, d, u, h, q] = g_out[lo:lo + 32]
            at = pl.multiple_of(16 * q, 16)
            for y in range(nmp):
                both = jnp.concatenate([kept[0][8 * y:8 * y + 8], kept[1][8 * y:8 * y + 8]], axis=0)
                terms[p, y, pl.ds(at, 16), :] = both.astype(BF16)

    def remote(src, dst, send, recv, target):
        return pltpu.make_async_remote_copy(
            src_ref=src, dst_ref=dst, send_sem=send, recv_sem=recv,
            device_id=target, device_id_type=MESH)

    def copy_a(k):
        return remote(part.at[k, 1 - c], from_core.at[k], a_send.at[k], a_recv.at[k], partner)

    def copies_b(k):
        out = [remote(pair.at[k, xl, 1 - xh], from_x.at[k, 0], b_send.at[k, 0], b_recv.at[k, 0], across)]
        for h in range(2):
            out.append(remote(pair.at[k, 1 - xl, h], from_x.at[k, 1 + xh],
                              b_send.at[k, 1 + h], b_recv.at[k, 1 + xh], sides[h]))
        return out

    def wait_b(k):
        for i in range(3):
            remote(from_x.at[k, i], from_x.at[k, i], b_send.at[k, i], b_recv.at[k, i], across).wait_recv()

    def copy_c(k, to):
        return remote(ready.at[k, to], landed.at[k, z], c_send.at[k, to], c_recv.at[k, z],
                      dev(2 * to + xl, r, m))

    def arrived_c(k, origin):
        return remote(landed.at[k, origin], landed.at[k, origin], c_send.at[k, origin], c_recv.at[k, origin], partner)

    def copy_t(p, to):
        return remote(terms.at[p, to], got.at[p, m], t_send.at[p, to], t_recv.at[p, m], dev(s, r, to))

    def arrived_t(p, origin):
        return remote(got.at[p, origin], got.at[p, origin], t_send.at[p, origin], t_recv.at[p, origin], partner)

    def copy_k(to):
        return remote(code, codes.at[m], k_send.at[to], k_recv.at[m], dev(s, r, to))

    def arrived_k(origin):
        return remote(codes.at[origin], codes.at[origin], k_send.at[origin], k_recv.at[origin], partner)

    def send_terms(p):
        @pl.loop(0, nmp - 1)
        def _(k):
            copy_t(p, along_y(k)).start()
        got[p, m] = terms[p, m]

    def add_pair(k):
        copy_a(k).wait_recv()

        @pl.loop(0, nz)
        def _(q):
            for u in range(2):
                for h in range(2):
                    pair[k, u, h, q] = (part[k, c, u, h, q].astype(F32) + from_core[k, u, h, q].astype(F32)).astype(BF16)
        for copy in copies_b(k):
            copy.start()

    def add_x(k):
        wait_b(k)

        @pl.loop(0, nz)
        def _(q):
            ready[k, q, xl] = (pair[k, xl, xh, q].astype(F32) + from_x[k, 0, q].astype(F32)).astype(BF16)
            ready[k, q, 1 - xl] = (from_x[k, 1, q].astype(F32) + from_x[k, 2, q].astype(F32)).astype(BF16)

        @pl.loop(0, nz - 1)
        def _(i):
            copy_c(k, along_z(i)).start()
        landed[k, z] = ready[k, z]

    for load in loads[0]:
        load.wait()
    compute(0)
    pl.semaphore_wait(barrier, 6 + (nz - 1) + (nmp - 1))
    copy_a(0).start()
    copy_a(1).start()

    @pl.loop(0, nmp - 1)
    def _(k):
        copy_k(along_y(k)).start()
    codes[m] = code[...]
    send_terms(0)

    for load in loads[1]:
        load.wait()
    compute(1)
    copy_a(2).start()
    copy_a(3).start()
    send_terms(1)

    for k in range(4):
        add_pair(k)
    for k in range(4):
        add_x(k)

    @pl.loop(0, nmp - 1)
    def _(i):
        arrived_k(along_y(i)).wait_recv()

    first = pl.multiple_of(16 * (m // 2), 16)
    odd = lax.rem(m, 2) == 1
    row = lax.broadcasted_iota(jnp.int32, (8, 128), 0) + 8 * m
    span = 8 * ns
    tile = 8 * count // 6 if (8 * count) % 96 == 0 else 8 * count
    for p in range(2):
        @pl.loop(0, nmp - 1)
        def _(i):
            arrived_t(p, along_y(i)).wait_recv()

        @pl.loop(0, 8 * count // tile)
        def _(i):
            base = i * tile
            place = lax.broadcasted_iota(jnp.int32, (tile, span), 0) + base
            total = jnp.zeros((tile, 128), F32)
            for y in range(nmp):
                hot = (place == codes[y, p:p + 1, :span]).astype(F32).astype(BF16)
                total = total + contract(hot, got[p, y], 1, 0)
            for b in range(tile // 8):
                at = pl.multiple_of(base * 16 + b * 128, 128)
                mine = gs[p][pl.ds(first, 16), pl.ds(at, 128)].astype(F32)
                mine = jnp.where(odd, mine[8:16], mine[0:8])
                mine = jnp.where(row < len_ref[p], mine, 0.0)
                dx[p, :, pl.ds(at, 128)] = (mine + total[8 * b:8 * b + 8]).astype(BF16)

        remote(dx.at[p], dx_in.at[p], d_send.at[p], d_recv.at[p], (down, up)[p]).start()

    for k in range(4):
        @pl.loop(0, nz - 1)
        def _(i):
            arrived_c(k, along_z(i)).wait_recv()

    @pl.loop(0, nz)
    def _(q):
        for kind in range(2):
            for u in range(2):
                grads_ref[2 * q + u, kind] = (landed[kind, q, u].astype(F32)
                                              + landed[2 + kind, nz - 1 - q, 1 - u].astype(F32))

    for p in range(2):
        remote(dx.at[p], dx_in.at[p], d_send.at[p], d_recv.at[p], (down, up)[p]).wait_recv()
        edge = s == (ns - 1 if p == 0 else 0)
        taken = dx_in[p]
        passed_ref[p] = jnp.where(edge, jnp.zeros_like(taken), taken)

    for k in range(4):
        copy_a(k).wait_send()
        for copy in copies_b(k):
            copy.wait_send()

        @pl.loop(0, nz - 1)
        def _(i):
            copy_c(k, along_z(i)).wait_send()

    @pl.loop(0, nmp - 1)
    def _(i):
        copy_k(along_y(i)).wait_send()
        for p in range(2):
            copy_t(p, along_y(i)).wait_send()
    for p in range(2):
        remote(dx.at[p], dx_in.at[p], d_send.at[p], d_recv.at[p], (down, up)[p]).wait_send()


def body(section_in, out_grad, lengths, w_in, w_out, idx_in, idx_out):
    x = section_in[:, 0]
    g = out_grad[:, 0]
    rows, width = x.shape[1:]
    nf = w_in.shape[2]
    nz = lax.axis_size("section") // 2
    nmp = lax.axis_size("mp")
    wide = -(-8 * nf // 128) * 128
    quad = (2, 2, nz, 32, 128)
    dma = pltpu.SemaphoreType.DMA
    smem = pl.BlockSpec(memory_space=pltpu.SMEM)
    anywhere = pl.BlockSpec(memory_space=pl.ANY)
    vmem = pl.BlockSpec(memory_space=pltpu.VMEM)
    passed, grads = pl.pallas_call(
        functools.partial(kernel, nz, nmp),
        out_shape=(
            jax.ShapeDtypeStruct((2, 8, width), BF16),
            jax.ShapeDtypeStruct((nf, 2, 32, 128), F32),
        ),
        in_specs=[smem] * 3 + [anywhere] * 4,
        out_specs=(vmem, vmem),
        scratch_shapes=[
            pltpu.VMEM((rows, width), BF16),
            pltpu.VMEM((rows, width), BF16),
            pltpu.VMEM((rows, width), BF16),
            pltpu.VMEM((rows, width), BF16),
            pltpu.VMEM((2, nf, 128, 128), BF16),
            pltpu.VMEM((2, nf, 128, 128), BF16),
            pltpu.VMEM((4, 2) + quad, BF16),
            pltpu.VMEM((4,) + quad, BF16),
            pltpu.VMEM((4,) + quad, BF16),
            pltpu.VMEM((4, 3, nz, 32, 128), BF16),
            pltpu.VMEM((4, nz, 2, 32, 128), BF16),
            pltpu.VMEM((4, nz, 2, 32, 128), BF16),
            pltpu.VMEM((2, nmp, 8 * nf, 128), BF16),
            pltpu.VMEM((2, nmp, 8 * nf, 128), BF16),
            pltpu.VMEM((8, wide), jnp.int32),
            pltpu.VMEM((nmp, 8, wide), jnp.int32),
            pltpu.VMEM((2, 8, width), BF16),
            pltpu.VMEM((2, 8, width), BF16),
            dma((2, 4)), dma((4,)), dma((4,)), dma((4, 3)), dma((4, 3)),
            dma((4, nz)), dma((4, nz)), dma((2, nmp)), dma((2, nmp)),
            dma((nmp,)), dma((nmp,)), dma((2,)), dma((2,)),
        ],
        compiler_params=pltpu.CompilerParams(
            collective_id=0, has_side_effects=True, vmem_limit_bytes=60 * 2**20),
    )(lengths[:, 0, 0], idx_in[0], idx_out[0], x, g, w_in[0], w_out[0])
    return passed[:, None], grads[:, :, None, None]


def solution(mesh):
    placed = (
        P(None, "section", "dp", None),
        P(None, "section", "dp", None),
        P(None, "section", "dp"),
        P("section", None, "mp", None, None),
        P("section", None, "mp", None, None),
        P("section", None, "mp"),
        P("section", None, "mp"),
    )
    return jax.shard_map(
        body,
        mesh=mesh,
        in_specs=placed,
        out_specs=(
            P(None, "section", ("dp", "mp"), None),
            P(None, None, "mp", "section", "dp", None),
        ),
        check_vma=False,
    )
```

```python
import functools

import jax
import jax.numpy as jnp
from jax import lax
from jax.experimental import pallas as pl
from jax.experimental.pallas import tpu as pltpu
from jax.sharding import PartitionSpec as P

MESH = pl.DeviceIdType.MESH
F32 = jnp.float32
BF16 = jnp.bfloat16
ROOT = 0.7978845608028654
CUBIC = 0.044715
PER = 4


def contract(a, b, da, db):
    return lax.dot_general(a, b, (((da,), (db,)), ((), ())), preferred_element_type=F32)


def kernel(
    nz, nmp, groups,
    len_hbm, ii_hbm, io_hbm, x_hbm, g_hbm, wi_hbm, wo_hbm,
    passed_ref, grads_ref,
    len_ref, ii_ref, io_ref,
    x0, x1, g0, g1, wiv, wov, part, from_core, pair, from_x, ready, landed,
    terms, got, code, codes, dx, dx_in,
    in_sem, int_sem, a_send, a_recv, b_send, b_recv, c_send, c_recv,
    t_send, t_recv, k_send, k_recv, d_send, d_recv,
):
    ns = 2 * nz
    size = nz // groups
    chunks = 2 * groups
    s = lax.axis_index("section")
    r = lax.axis_index("dp")
    m = lax.axis_index("mp")
    z, xl = s // 2, lax.rem(s, 2)
    xh, c = r // 2, lax.rem(r, 2)
    rows, width = x0.shape
    count = width // 128
    xs, gs = (x0, x1), (g0, g1)

    def dev(section, dp, mp):
        return {"section": section, "dp": dp, "mp": mp}

    partner = dev(s, 2 * xh + (1 - c), m)
    across = dev(s, 2 * (1 - xh) + c, m)
    sides = [dev(2 * z + (1 - xl), 2 * h + c, m) for h in range(2)]
    down = dev(lax.rem(s + ns - 1, ns), r, m)
    up = dev(lax.rem(s + 1, ns), r, m)

    def spread(me, n, k):
        to = jnp.where(lax.rem(k, 2) == 0, me + (n // 2 - k // 2), me - (n // 2 - (k + 1) // 2))
        return lax.rem(to + n, n)

    def along_z(k):
        return spread(z, nz, k)

    def along_y(k):
        return spread(m, nmp, k)

    ints = [
        pltpu.make_async_copy(ii_hbm, ii_ref, int_sem.at[0]),
        pltpu.make_async_copy(io_hbm, io_ref, int_sem.at[1]),
        pltpu.make_async_copy(len_hbm, len_ref, int_sem.at[2]),
    ]
    for load in ints:
        load.start()
    loads = []
    for p in range(2):
        loads.append([
            pltpu.make_async_copy(x_hbm.at[p], xs[p], in_sem.at[p, 0]),
            pltpu.make_async_copy(wi_hbm.at[p], wiv.at[p], in_sem.at[p, 1]),
            pltpu.make_async_copy(g_hbm.at[p], gs[p], in_sem.at[p, 2]),
            pltpu.make_async_copy(wo_hbm.at[p], wov.at[p], in_sem.at[p, 3]),
        ])
        for load in loads[p]:
            load.start()

    barrier = pltpu.get_barrier_semaphore()

    def greet(target):
        pl.semaphore_signal(barrier, inc=1, device_id=target, device_id_type=MESH)

    @pl.loop(0, nz - 1)
    def _(k):
        greet(dev(2 * along_z(k) + xl, r, m))

    @pl.loop(0, nmp - 1)
    def _(k):
        greet(dev(s, r, along_y(k)))

    for target in [partner, across, sides[0], sides[1], down, up]:
        greet(target)

    for load in ints:
        load.wait()

    wide = code.shape[1]
    lane = lax.broadcasted_iota(jnp.int32, (8, wide), 1)
    relay = lax.broadcasted_iota(jnp.int32, (8, wide), 0)
    value = jnp.full((8, wide), -1, jnp.int32)
    for j in range(2 * nz):
        chosen = jnp.where(relay == 0, ii_ref[0, j], ii_ref[1, j])
        value = jnp.where(lane // 8 == j, chosen * 8 + lane % 8, value)
    code[...] = value

    def compute(n):
        p, g = n // groups, n % groups
        live = lax.broadcasted_iota(jnp.int32, (rows, 128), 0) < len_ref[p]
        for t0 in range(0, size, PER):
            slots = list(range(t0, min(t0 + PER, size)))
            qs = {t: along_z(g * size + t) for t in slots}
            items = [(t, u) for t in slots for u in range(2)]
            x, back, wi, wo, pre, back_pre, act, grad, term = ({} for _ in range(9))
            for i in items:
                j = 2 * qs[i[0]] + i[1]
                x[i] = xs[p][:, pl.ds(ii_ref[p, j] * 128, 128)]
                wi[i] = wiv[p, j]
                pre[i] = contract(x[i], wi[i], 1, 0)
            for i in items:
                j = 2 * qs[i[0]] + i[1]
                picked = gs[p][:, pl.ds(io_ref[p, j] * 128, 128)]
                back[i] = jnp.where(live, picked.astype(F32), 0.0).astype(BF16)
                wo[i] = wov[p, j]
                back_pre[i] = contract(back[i], wo[i], 1, 1)
            for i in items:
                v = pre[i]
                square = v * v
                th = jnp.tanh(ROOT * (v + CUBIC * (square * v)))
                half = 0.5 * (1.0 + th)
                act[i] = (v * half).astype(BF16)
                slope = half + (0.5 * v) * (1.0 - th * th) * (ROOT * (1.0 + (3.0 * CUBIC) * square))
                grad[i] = (back_pre[i] * slope).astype(BF16)
            for i in items:
                t, u = i
                outs = (contract(x[i], grad[i], 0, 0).astype(BF16), contract(act[i], back[i], 0, 0).astype(BF16))
                for kind in range(2):
                    for h in range(2):
                        for d in range(2):
                            lo = 32 * (2 * h + d)
                            part[n, d, u, h, t, kind] = outs[kind][lo:lo + 32]
                term[i] = contract(grad[i], wi[i], 1, 1)
            for t in slots:
                at = pl.multiple_of(16 * qs[t], 16)
                for y in range(nmp):
                    both = jnp.concatenate([term[t, 0][8 * y:8 * y + 8], term[t, 1][8 * y:8 * y + 8]], axis=0)
                    terms[p, y, pl.ds(at, 16), :] = both.astype(BF16)

    def remote(src, dst, send, recv, target):
        return pltpu.make_async_remote_copy(
            src_ref=src, dst_ref=dst, send_sem=send, recv_sem=recv,
            device_id=target, device_id_type=MESH)

    def copy_a(n):
        return remote(part.at[n, 1 - c], from_core.at[n], a_send.at[n], a_recv.at[n], partner)

    def copies_b(n):
        out = [remote(pair.at[n, xl, 1 - xh], from_x.at[n, 0], b_send.at[n, 0], b_recv.at[n, 0], across)]
        for h in range(2):
            out.append(remote(pair.at[n, 1 - xl, h], from_x.at[n, 1 + xh],
                              b_send.at[n, 1 + h], b_recv.at[n, 1 + xh], sides[h]))
        return out

    def copy_c(n, t):
        p, g = n // groups, n % groups
        to = along_z(g * size + t)
        return remote(ready.at[n, t], landed.at[p, z], c_send.at[n, t], c_recv.at[p, z],
                      dev(2 * to + xl, r, m))

    def arrived_c(p, origin):
        return remote(landed.at[p, origin], landed.at[p, origin], c_send.at[0, 0], c_recv.at[p, origin], partner)

    def copy_t(p, to):
        return remote(terms.at[p, to], got.at[p, m], t_send.at[p, to], t_recv.at[p, m], dev(s, r, to))

    def arrived_t(p, origin):
        return remote(got.at[p, origin], got.at[p, origin], t_send.at[p, origin], t_recv.at[p, origin], partner)

    def copy_k(to):
        return remote(code, codes.at[m], k_send.at[to], k_recv.at[m], dev(s, r, to))

    def arrived_k(origin):
        return remote(codes.at[origin], codes.at[origin], k_send.at[origin], k_recv.at[origin], partner)

    def copy_d(p):
        return remote(dx.at[p], dx_in.at[p], d_send.at[p], d_recv.at[p], (down, up)[p])

    def send_terms(p):
        @pl.loop(0, nmp - 1)
        def _(k):
            copy_t(p, along_y(k)).start()
        got[p, m] = terms[p, m]

    def add_pair(n):
        copy_a(n).wait_recv()
        copies = copies_b(n)
        for u in range(2):
            for h in range(2):
                pair[n, u, h] = part[n, c, u, h] + from_core[n, u, h]
        for copy in copies:
            copy.start()

    def add_x(n):
        for i in range(3):
            remote(from_x.at[n, i], from_x.at[n, i], b_send.at[n, i], b_recv.at[n, i], across).wait_recv()
        g = n % groups
        last = size - 1 if g == groups - 1 else size
        for t in range(size):
            ready[n, t, xl] = pair[n, xl, xh, t] + from_x[n, 0, t]
            ready[n, t, 1 - xl] = from_x[n, 1, t] + from_x[n, 2, t]
            if t < last:
                copy_c(n, t).start()
        if g == groups - 1:
            landed[n // groups, z] = ready[n, size - 1]

    def scatter(p):
        first = pl.multiple_of(16 * (m // 2), 16)
        odd = lax.rem(m, 2) == 1
        row = lax.broadcasted_iota(jnp.int32, (8, 128), 0) + 8 * m
        span = 8 * ns
        tile = 8 * count // 3 if (8 * count) % 96 == 0 else 8 * count

        @pl.loop(0, nmp - 1)
        def _(i):
            arrived_t(p, along_y(i)).wait_recv()

        @pl.loop(0, 8 * count // tile)
        def _(i):
            base = i * tile
            place = lax.broadcasted_iota(jnp.int32, (tile, span), 0) + base
            total = jnp.zeros((tile, 128), F32)
            for y in range(nmp):
                hot = (place == codes[y, p:p + 1, :span]).astype(F32).astype(BF16)
                total = total + contract(hot, got[p, y], 1, 0)
            for b in range(tile // 8):
                at = pl.multiple_of(base * 16 + b * 128, 128)
                mine = gs[p][pl.ds(first, 16), pl.ds(at, 128)].astype(F32)
                mine = jnp.where(odd, mine[8:16], mine[0:8])
                mine = jnp.where(row < len_ref[p], mine, 0.0)
                dx[p, :, pl.ds(at, 128)] = (mine + total[8 * b:8 * b + 8]).astype(BF16)
        copy_d(p).start()

    for load in loads[0]:
        load.wait()
    early = min(2, groups)
    for n in range(early):
        compute(n)
    pl.semaphore_wait(barrier, 6 + (nz - 1) + (nmp - 1))
    for n in range(early):
        copy_a(n).start()

    @pl.loop(0, nmp - 1)
    def _(k):
        copy_k(along_y(k)).start()
    codes[m] = code[...]
    if early == groups:
        send_terms(0)
    for n in range(early, chunks):
        if n == groups:
            for load in loads[1]:
                load.wait()
        compute(n)
        copy_a(n).start()
        if n % groups == groups - 1:
            send_terms(n // groups)
        add_pair(n - early)
    moved = 0
    for n in range(chunks - early, chunks):
        add_x(moved)
        moved += 1
        add_pair(n)
    for n in range(moved, chunks):
        add_x(n)

    @pl.loop(0, nmp - 1)
    def _(i):
        arrived_k(along_y(i)).wait_recv()
    for p in range(2):
        scatter(p)

    for n in range(chunks):
        copy_a(n).wait_send()
        for copy in copies_b(n):
            copy.wait_send()

    @pl.loop(0, nmp - 1)
    def _(i):
        copy_k(along_y(i)).wait_send()
        for p in range(2):
            copy_t(p, along_y(i)).wait_send()

    def take(p):
        copy_d(p).wait_recv()
        edge = s == (ns - 1 if p == 0 else 0)
        taken = dx_in[p]
        passed_ref[p] = jnp.where(edge, jnp.zeros_like(taken), taken)

    def total(o):
        q = nz - 1 - o
        for u in range(2):
            for kind in range(2):
                grads_ref[2 * q + u, kind] = (landed[0, q, u, kind].astype(F32)
                                              + landed[1, o, 1 - u, kind].astype(F32))

    @pl.loop(0, nz - 1)
    def _(k):
        arrived_c(0, along_z(k)).wait_recv()
    total(z)
    take(0)

    @pl.loop(0, nz - 1)
    def _(k):
        o = along_z(k)
        arrived_c(1, o).wait_recv()
        total(o)
    take(1)

    for n in range(chunks):
        last = size - 1 if n % groups == groups - 1 else size

        @pl.loop(0, last)
        def _(t):
            copy_c(n, t).wait_send()
    for p in range(2):
        copy_d(p).wait_send()


def body(section_in, out_grad, lengths, w_in, w_out, idx_in, idx_out):
    x = section_in[:, 0]
    g = out_grad[:, 0]
    rows, width = x.shape[1:]
    nf = w_in.shape[2]
    nz = lax.axis_size("section") // 2
    nmp = lax.axis_size("mp")
    wide = -(-8 * nf // 128) * 128
    groups = 3 if nz % 3 == 0 else 1
    chunks, size = 2 * groups, nz // groups
    dma = pltpu.SemaphoreType.DMA
    hbm = pl.BlockSpec(memory_space=pltpu.HBM)
    vmem = pl.BlockSpec(memory_space=pltpu.VMEM)
    slab = (size, 2, 32, 128)
    passed, grads = pl.pallas_call(
        functools.partial(kernel, nz, nmp, groups),
        out_shape=(
            jax.ShapeDtypeStruct((2, 8, width), BF16),
            jax.ShapeDtypeStruct((nf, 2, 32, 128), F32),
        ),
        in_specs=[hbm] * 7,
        out_specs=(vmem, vmem),
        scratch_shapes=[
            pltpu.SMEM((2,), jnp.int32),
            pltpu.SMEM((2, nf), jnp.int32),
            pltpu.SMEM((2, nf), jnp.int32),
            pltpu.VMEM((rows, width), BF16),
            pltpu.VMEM((rows, width), BF16),
            pltpu.VMEM((rows, width), BF16),
            pltpu.VMEM((rows, width), BF16),
            pltpu.VMEM((2, nf, 128, 128), BF16),
            pltpu.VMEM((2, nf, 128, 128), BF16),
            pltpu.VMEM((chunks, 2, 2, 2) + slab, BF16),
            pltpu.VMEM((chunks, 2, 2) + slab, BF16),
            pltpu.VMEM((chunks, 2, 2) + slab, BF16),
            pltpu.VMEM((chunks, 3) + slab, BF16),
            pltpu.VMEM((chunks, size, 2, 2, 32, 128), BF16),
            pltpu.VMEM((2, nz, 2, 2, 32, 128), BF16),
            pltpu.VMEM((2, nmp, 8 * nf, 128), BF16),
            pltpu.VMEM((2, nmp, 8 * nf, 128), BF16),
            pltpu.VMEM((8, wide), jnp.int32),
            pltpu.VMEM((nmp, 8, wide), jnp.int32),
            pltpu.VMEM((2, 8, width), BF16),
            pltpu.VMEM((2, 8, width), BF16),
            dma((2, 4)), dma((3,)), dma((chunks,)), dma((chunks,)), dma((chunks, 3)), dma((chunks, 3)),
            dma((chunks, size)), dma((2, nz)), dma((2, nmp)), dma((2, nmp)),
            dma((nmp,)), dma((nmp,)), dma((2,)), dma((2,)),
        ],
        compiler_params=pltpu.CompilerParams(
            collective_id=0, has_side_effects=True, vmem_limit_bytes=56 * 2**20),
    )(lengths[:, 0, 0], idx_in[0], idx_out[0], x, g, w_in[0], w_out[0])
    return passed[:, None], grads[:, :, None, None]


def solution(mesh):
    placed = (
        P(None, "section", "dp", None),
        P(None, "section", "dp", None),
        P(None, "section", "dp"),
        P("section", None, "mp", None, None),
        P("section", None, "mp", None, None),
        P("section", None, "mp"),
        P("section", None, "mp"),
    )
    return jax.shard_map(
        body,
        mesh=mesh,
        in_specs=placed,
        out_specs=(
            P(None, "section", ("dp", "mp"), None),
            P(None, None, "mp", "section", "dp", None),
        ),
        check_vma=False,
    )
```

```python
import functools

import jax
import jax.numpy as jnp
from jax import lax
from jax.experimental import pallas as pl
from jax.experimental.pallas import tpu as pltpu
from jax.sharding import PartitionSpec as P

MESH = pl.DeviceIdType.MESH
F32 = jnp.float32
BF16 = jnp.bfloat16
ROOT = 0.7978845608028654
CUBIC = 0.044715
PER = 4
HEAD = 1


def contract(a, b, da, db):
    return lax.dot_general(a, b, (((da,), (db,)), ((), ())), preferred_element_type=F32)


def kernel(
    nz, nmp, groups,
    tab_hbm, x_hbm, g_hbm, wi_hbm, wo_hbm,
    passed_ref, grads_ref,
    tab,
    x0, x1, g0, g1, wiv, wov, part, from_core, pair, from_x, ready, landed,
    terms, got, code, codes, dx, dx_in, hop,
    in_sem, int_sem, a_send, a_recv, b_send, b_recv, c_send, c_recv,
    t_send, t_recv, k_send, k_recv, d_send, d_recv, e_send, e_recv, h_send, h_recv, above, above_cross,
):
    ns = 2 * nz
    size = nz // groups
    chunks = 2 * groups
    s = lax.axis_index("section")
    r = lax.axis_index("dp")
    m = lax.axis_index("mp")
    z, xl = s // 2, lax.rem(s, 2)
    xh, c = r // 2, lax.rem(r, 2)
    rows, width = x0.shape
    count = width // 128
    xs, gs = (x0, x1), (g0, g1)

    def dev(section, dp, mp):
        return {"section": section, "dp": dp, "mp": mp}

    partner = dev(s, 2 * xh + (1 - c), m)
    across = dev(s, 2 * (1 - xh) + c, m)
    sides = [dev(2 * z + (1 - xl), 2 * h + c, m) for h in range(2)]
    down = dev(lax.rem(s + ns - 1, ns), r, m)
    up = dev(lax.rem(s + 1, ns), r, m)

    def spread(me, n, k):
        to = jnp.where(lax.rem(k, 2) == 0, me + (n // 2 - k // 2), me - (n // 2 - (k + 1) // 2))
        return lax.rem(to + n, n)

    def along_z(k):
        return spread(z, nz, k)

    def along_y(k):
        return spread(m, nmp, k)

    table = pltpu.make_async_copy(tab_hbm, tab, int_sem)
    table.start()
    loads = []
    for p in range(2):
        loads.append([
            pltpu.make_async_copy(x_hbm.at[p], xs[p], in_sem.at[p, 0]),
            pltpu.make_async_copy(wi_hbm.at[p], wiv.at[p], in_sem.at[p, 1]),
            pltpu.make_async_copy(g_hbm.at[p], gs[p], in_sem.at[p, 2]),
            pltpu.make_async_copy(wo_hbm.at[p], wov.at[p], in_sem.at[p, 3]),
        ])

    for load in loads[0]:
        load.start()

    barrier = pltpu.get_barrier_semaphore()

    def greet(target):
        pl.semaphore_signal(barrier, inc=1, device_id=target, device_id_type=MESH)

    cross = jnp.where(xl == 0, lax.rem(s + ns - 1, ns), lax.rem(s + 1, ns))
    cross_above = cross // 2 > z

    def in_column(k):
        to = along_z(k)
        return to, dev(2 * to + xl, r, m)

    for target in [partner, across, sides[0], sides[1]]:
        greet(target)

    @pl.loop(0, nmp - 1)
    def _(k):
        greet(dev(s, r, along_y(k)))

    @pl.loop(0, nz - 1)
    def _(k):
        to, target = in_column(k)

        @pl.when(to > z)
        def _():
            greet(target)

    @pl.when(cross_above)
    def _():
        greet(dev(cross, r, m))

    def enter():
        pl.semaphore_wait(barrier, 4 + (nmp - 1) + z + jnp.where(cross_above, 0, 1))

        @pl.loop(0, nz - 1)
        def _(k):
            to, target = in_column(k)

            @pl.when(to < z)
            def _():
                pl.semaphore_signal(above.at[z], inc=1, device_id=target, device_id_type=MESH)

        @pl.when(jnp.logical_not(cross_above))
        def _():
            pl.semaphore_signal(above_cross, inc=1, device_id=dev(cross, r, m), device_id_type=MESH)

    table.wait()

    wide = code.shape[1]
    lane = lax.broadcasted_iota(jnp.int32, (8, wide), 1)
    relay = lax.broadcasted_iota(jnp.int32, (8, wide), 0)
    value = jnp.full((8, wide), -1, jnp.int32)
    for j in range(2 * nz):
        chosen = jnp.where(relay == 0, tab[0, j] >> 20, tab[1, j] >> 20)
        value = jnp.where(lane // 8 == j, chosen * 8 + lane % 8, value)
    code[...] = value

    def compute(p, slots):
        live = lax.broadcasted_iota(jnp.int32, (rows, 128), 0) < (tab[p, 0] & 255)
        if slots:
            qs = {t: along_z(t) for t in slots}
            items = [(t, u) for t in slots for u in range(2)]
            x, back, wi, wo, pre, back_pre, act, grad, term = ({} for _ in range(9))
            for i in items:
                j = 2 * qs[i[0]] + i[1]
                x[i] = xs[p][:, pl.ds((tab[p, j] >> 20) * 128, 128)]
                wi[i] = wiv[p, j]
                pre[i] = contract(x[i], wi[i], 1, 0)
            for i in items:
                j = 2 * qs[i[0]] + i[1]
                picked = gs[p][:, pl.ds(((tab[p, j] >> 8) & 4095) * 128, 128)]
                back[i] = jnp.where(live, picked.astype(F32), 0.0).astype(BF16)
                wo[i] = wov[p, j]
                back_pre[i] = contract(back[i], wo[i], 1, 1)
            for i in items:
                v = pre[i]
                square = v * v
                th = jnp.tanh(ROOT * (v + CUBIC * (square * v)))
                half = 0.5 * (1.0 + th)
                act[i] = (v * half).astype(BF16)
                slope = half + (0.5 * v) * (1.0 - th * th) * (ROOT * (1.0 + (3.0 * CUBIC) * square))
                grad[i] = (back_pre[i] * slope).astype(BF16)
            for i in items:
                t, u = i
                outs = (contract(x[i], grad[i], 0, 0).astype(BF16), contract(act[i], back[i], 0, 0).astype(BF16))
                for kind in range(2):
                    for h in range(2):
                        for d in range(2):
                            lo = 32 * (2 * h + d)
                            part[p * groups + t // size, d, u, h, t % size, kind] = outs[kind][lo:lo + 32]
                term[i] = contract(grad[i], wi[i], 1, 1)
            for t in slots:
                at = pl.multiple_of(16 * qs[t], 16)
                for y in range(nmp):
                    both = jnp.concatenate([term[t, 0][8 * y:8 * y + 8], term[t, 1][8 * y:8 * y + 8]], axis=0)
                    terms[p, y, pl.ds(at, 16), :] = both.astype(BF16)

    def remote(src, dst, send, recv, target):
        return pltpu.make_async_remote_copy(
            src_ref=src, dst_ref=dst, send_sem=send, recv_sem=recv,
            device_id=target, device_id_type=MESH)

    def copy_a(n):
        return remote(part.at[n, 1 - c], from_core.at[n], a_send.at[n], a_recv.at[n], partner)

    def copies_b(n):
        out = [remote(pair.at[n, xl, 1 - xh], from_x.at[n, 0], b_send.at[n, 0], b_recv.at[n, 0], across)]
        for h in range(2):
            out.append(remote(pair.at[n, 1 - xl, h], from_x.at[n, 1 + xh],
                              b_send.at[n, 1 + h], b_recv.at[n, 1 + xh], sides[h]))
        return out

    def copy_c(n, t):
        p, g = n // groups, n % groups
        to = along_z(g * size + t)
        return remote(ready.at[n, t], landed.at[p, z], c_send.at[n, t], c_recv.at[p, z],
                      dev(2 * to + xl, r, m))

    def arrived_c(p, origin):
        return remote(landed.at[p, origin], landed.at[p, origin], c_send.at[0, 0], c_recv.at[p, origin], partner)

    def copy_t(p, to):
        return remote(terms.at[p, to], got.at[p, m], t_send.at[p, to], t_recv.at[p, m], dev(s, r, to))

    def arrived_t(p, origin):
        return remote(got.at[p, origin], got.at[p, origin], t_send.at[p, origin], t_recv.at[p, origin], partner)

    def copy_k(to):
        return remote(code, codes.at[m], k_send.at[to], k_recv.at[m], dev(s, r, to))

    def arrived_k(origin):
        return remote(codes.at[origin], codes.at[origin], k_send.at[origin], k_recv.at[origin], partner)

    cut = width // 2
    back_turn = jnp.where(xl == 0, 2, ns - 2)
    side = dev(2 * z + (1 - xl), r, m)
    along = dev(lax.rem(s + back_turn, ns), r, m)

    def copy_d(p):
        return remote(dx.at[p, :, :cut], dx_in.at[p, :, :cut], d_send.at[p], d_recv.at[p], (down, up)[p])

    def copy_e():
        return remote(dx.at[1 - xl, :, cut:], dx_in.at[1 - xl, :, cut:], e_send, e_recv.at[1 - xl], side)

    def copy_hop():
        return remote(dx.at[xl, :, cut:], hop, h_send.at[0], h_recv, side)

    def forward():
        return remote(hop, dx_in.at[1 - xl, :, cut:], h_send.at[1], e_recv.at[1 - xl], along)

    def arrived_e(p):
        return remote(dx_in.at[p, :, cut:], dx_in.at[p, :, cut:], e_send, e_recv.at[p], partner)

    def send_terms(p):
        @pl.loop(0, nmp - 1)
        def _(k):
            copy_t(p, along_y(k)).start()
        got[p, m] = terms[p, m]

    def add_pair(n):
        copy_a(n).wait_recv()
        copies = copies_b(n)
        for u in range(2):
            for h in range(2):
                pair[n, u, h] = part[n, c, u, h] + from_core[n, u, h]
        for copy in copies:
            copy.start()

    def add_x(n):
        for i in range(3):
            remote(from_x.at[n, i], from_x.at[n, i], b_send.at[n, i], b_recv.at[n, i], across).wait_recv()
        g = n % groups
        last = size - 1 if g == groups - 1 else size
        for t in range(size):
            ready[n, t, xl] = pair[n, xl, xh, t] + from_x[n, 0, t]
            ready[n, t, 1 - xl] = from_x[n, 1, t] + from_x[n, 2, t]
            if t < last:
                if n < groups:
                    to = along_z(g * size + t)

                    @pl.when(to > z)
                    def _():
                        pl.semaphore_wait(above.at[to], 1)
                copy_c(n, t).start()
        if g == groups - 1:
            landed[n // groups, z] = ready[n, size - 1]

    def scatter(p):
        first = pl.multiple_of(16 * (m // 2), 16)
        odd = lax.rem(m, 2) == 1
        row = lax.broadcasted_iota(jnp.int32, (8, 128), 0) + 8 * m
        span = 8 * ns
        tile = 8 * count // 3 if (8 * count) % 96 == 0 else 8 * count

        @pl.loop(0, nmp - 1)
        def _(i):
            arrived_t(p, along_y(i)).wait_recv()

        @pl.loop(0, 8 * count // tile)
        def _(i):
            base = i * tile
            place = lax.broadcasted_iota(jnp.int32, (tile, span), 0) + base
            total = jnp.zeros((tile, 128), F32)
            for y in range(nmp):
                hot = (place == codes[y, p:p + 1, :span]).astype(F32).astype(BF16)
                total = total + contract(hot, got[p, y], 1, 0)
            for b in range(tile // 8):
                at = pl.multiple_of(base * 16 + b * 128, 128)
                mine = gs[p][pl.ds(first, 16), pl.ds(at, 128)].astype(F32)
                mine = jnp.where(odd, mine[8:16], mine[0:8])
                mine = jnp.where(row < (tab[p, 0] & 255), mine, 0.0)
                dx[p, :, pl.ds(at, 128)] = (mine + total[8 * b:8 * b + 8]).astype(BF16)
        copy_d(p).start()

    steps = [(p, list(range(t, min(t + PER, nz)))) for p in range(2) for t in range(0, nz, PER)]
    half = len(steps) // 2
    early = 1

    def chunks_of(step):
        p, slots = step
        return sorted({p * groups + t // size for t in slots})

    for load in loads[0]:
        load.wait()
    for load in loads[1]:
        load.start()
    for step in steps[:early]:
        compute(*step)
    enter()
    for step in steps[:early]:
        for n in chunks_of(step):
            copy_a(n).start()

    @pl.loop(0, nmp - 1)
    def _(k):
        copy_k(along_y(k)).start()
    codes[m] = code[...]
    if early == half:
        send_terms(0)
    paired = moved = 0
    for i in range(early, len(steps)):
        if i == half:
            for load in loads[1]:
                load.wait()
        if HEAD and i == len(steps) - 1 and i > half:
            for _ in range(HEAD):
                add_x(moved)
                moved += 1
        compute(*steps[i])
        for n in chunks_of(steps[i]):
            copy_a(n).start()
        if i == half - 1:
            send_terms(0)
        while paired <= chunks_of(steps[i - 1])[-1]:
            add_pair(paired)
            paired += 1
    send_terms(1)
    lead = moved + 1
    while moved < chunks:
        if paired < chunks and moved >= lead:
            add_pair(paired)
            paired += 1
        add_x(moved)
        moved += 1

    @pl.loop(0, nmp - 1)
    def _(i):
        arrived_k(along_y(i)).wait_recv()
    @pl.when(cross_above)
    def _():
        pl.semaphore_wait(above_cross, 1)
    for p in range(2):
        scatter(p)
    copy_hop().start()
    copy_e().start()
    copy_hop().wait_recv()
    forward().start()

    for n in range(chunks):
        copy_a(n).wait_send()
        for copy in copies_b(n):
            copy.wait_send()

    @pl.loop(0, nmp - 1)
    def _(i):
        copy_k(along_y(i)).wait_send()
        for p in range(2):
            copy_t(p, along_y(i)).wait_send()

    def take(p):
        copy_d(p).wait_recv()
        arrived_e(p).wait_recv()
        edge = s == (ns - 1 if p == 0 else 0)
        taken = dx_in[p]
        passed_ref[p] = jnp.where(edge, jnp.zeros_like(taken), taken)

    def total(o):
        q = nz - 1 - o
        for u in range(2):
            for kind in range(2):
                grads_ref[2 * q + u, kind] = (landed[0, q, u, kind].astype(F32)
                                              + landed[1, o, 1 - u, kind].astype(F32))

    @pl.loop(0, nz - 1)
    def _(k):
        arrived_c(0, along_z(k)).wait_recv()
    total(z)
    take(0)

    @pl.loop(0, nz - 1)
    def _(k):
        o = along_z(k)
        arrived_c(1, o).wait_recv()
        total(o)
    take(1)

    for n in range(chunks):
        last = size - 1 if n % groups == groups - 1 else size

        @pl.loop(0, last)
        def _(t):
            copy_c(n, t).wait_send()
    for p in range(2):
        copy_d(p).wait_send()
    copy_e().wait_send()
    copy_hop().wait_send()
    forward().wait_send()


def body(section_in, out_grad, lengths, w_in, w_out, idx_in, idx_out):
    x = section_in[:, 0]
    g = out_grad[:, 0]
    rows, width = x.shape[1:]
    nf = w_in.shape[2]
    nz = lax.axis_size("section") // 2
    nmp = lax.axis_size("mp")
    wide = -(-8 * nf // 128) * 128
    groups = 6 if nz % 6 == 0 else 1
    chunks, size = 2 * groups, nz // groups
    dma = pltpu.SemaphoreType.DMA
    hbm = pl.BlockSpec(memory_space=pltpu.HBM)
    vmem = pl.BlockSpec(memory_space=pltpu.VMEM)
    slab = (size, 2, 32, 128)
    table = (idx_in[0] * 4096 + idx_out[0]) * 256 + lengths[:, 0]
    passed, grads = pl.pallas_call(
        functools.partial(kernel, nz, nmp, groups),
        out_shape=(
            jax.ShapeDtypeStruct((2, 8, width), BF16),
            jax.ShapeDtypeStruct((nf, 2, 32, 128), F32),
        ),
        in_specs=[hbm] * 5,
        out_specs=(vmem, vmem),
        scratch_shapes=[
            pltpu.SMEM((2, nf), jnp.int32),
            pltpu.VMEM((rows, width), BF16),
            pltpu.VMEM((rows, width), BF16),
            pltpu.VMEM((rows, width), BF16),
            pltpu.VMEM((rows, width), BF16),
            pltpu.VMEM((2, nf, 128, 128), BF16),
            pltpu.VMEM((2, nf, 128, 128), BF16),
            pltpu.VMEM((chunks, 2, 2, 2) + slab, BF16),
            pltpu.VMEM((chunks, 2, 2) + slab, BF16),
            pltpu.VMEM((chunks, 2, 2) + slab, BF16),
            pltpu.VMEM((chunks, 3) + slab, BF16),
            pltpu.VMEM((chunks, size, 2, 2, 32, 128), BF16),
            pltpu.VMEM((2, nz, 2, 2, 32, 128), BF16),
            pltpu.VMEM((2, nmp, 8 * nf, 128), BF16),
            pltpu.VMEM((2, nmp, 8 * nf, 128), BF16),
            pltpu.VMEM((8, wide), jnp.int32),
            pltpu.VMEM((nmp, 8, wide), jnp.int32),
            pltpu.VMEM((2, 8, width), BF16),
            pltpu.VMEM((2, 8, width), BF16),
            pltpu.VMEM((8, width // 2), BF16),
            dma((2, 4)), dma, dma((chunks,)), dma((chunks,)), dma((chunks, 3)), dma((chunks, 3)),
            dma((chunks, size)), dma((2, nz)), dma((2, nmp)), dma((2, nmp)),
            dma((nmp,)), dma((nmp,)), dma((2,)), dma((2,)), dma, dma((2,)), dma((2,)), dma,
            pltpu.SemaphoreType.REGULAR((nz,)), pltpu.SemaphoreType.REGULAR,
        ],
        compiler_params=pltpu.CompilerParams(
            collective_id=0, has_side_effects=True, vmem_limit_bytes=52 * 2**20),
    )(table, x, g, w_in[0], w_out[0])
    return passed[:, None], grads[:, :, None, None]


def solution(mesh):
    placed = (
        P(None, "section", "dp", None),
        P(None, "section", "dp", None),
        P(None, "section", "dp"),
        P("section", None, "mp", None, None),
        P("section", None, "mp", None, None),
        P("section", None, "mp"),
        P("section", None, "mp"),
    )
    return jax.shard_map(
        body,
        mesh=mesh,
        in_specs=placed,
        out_specs=(
            P(None, "section", ("dp", "mp"), None),
            P(None, None, "mp", "section", "dp", None),
        ),
        check_vma=False,
    )
```

```python
import functools

import jax
import jax.numpy as jnp
from jax import lax
from jax.experimental import pallas as pl
from jax.experimental.pallas import tpu as pltpu
from jax.sharding import PartitionSpec as P

MESH = pl.DeviceIdType.MESH
F32 = jnp.float32
BF16 = jnp.bfloat16
ROOT = 0.7978845608028654
CUBIC = 0.044715
PER = 4
HEAD = 1


def contract(a, b, da, db):
    return lax.dot_general(a, b, (((da,), (db,)), ((), ())), preferred_element_type=F32)


def kernel(
    nz, nmp, groups,
    tab_hbm, x_hbm, g_hbm, wi_hbm, wo_hbm,
    passed_ref, grads_ref,
    tab,
    x0, x1, g0, g1, wiv, wov, part, from_core, pair, from_x, ready, landed,
    terms, got, code, codes, dx, dx_in, hop,
    in_sem, int_sem, a_send, a_recv, b_send, b_recv, c_send, c_recv,
    t_send, t_recv, k_send, k_recv, d_send, d_recv, e_send, e_recv, h_send, h_recv, above, above_cross,
):
    ns = 2 * nz
    size = nz // groups
    chunks = 2 * groups
    s = lax.axis_index("section")
    r = lax.axis_index("dp")
    m = lax.axis_index("mp")
    z, xl = s // 2, lax.rem(s, 2)
    xh, c = r // 2, lax.rem(r, 2)
    rows, width = x0.shape
    count = width // 128
    xs, gs = (x0, x1), (g0, g1)

    def dev(section, dp, mp):
        return {"section": section, "dp": dp, "mp": mp}

    partner = dev(s, 2 * xh + (1 - c), m)
    across = dev(s, 2 * (1 - xh) + c, m)
    sides = [dev(2 * z + (1 - xl), 2 * h + c, m) for h in range(2)]
    down = dev(lax.rem(s + ns - 1, ns), r, m)
    up = dev(lax.rem(s + 1, ns), r, m)

    def spread(me, n, k):
        to = jnp.where(lax.rem(k, 2) == 0, me + (n // 2 - k // 2), me - (n // 2 - (k + 1) // 2))
        return lax.rem(to + n, n)

    def along_z(k):
        return spread(z, nz, k)

    def along_y(k):
        return spread(m, nmp, k)

    table = pltpu.make_async_copy(tab_hbm, tab, int_sem)
    table.start()
    loads = []
    for p in range(2):
        loads.append([
            pltpu.make_async_copy(x_hbm.at[p], xs[p], in_sem.at[p, 0]),
            pltpu.make_async_copy(wi_hbm.at[p], wiv.at[p], in_sem.at[p, 1]),
            pltpu.make_async_copy(g_hbm.at[p], gs[p], in_sem.at[p, 2]),
            pltpu.make_async_copy(wo_hbm.at[p], wov.at[p], in_sem.at[p, 3]),
        ])

    for load in loads[0]:
        load.start()

    barrier = pltpu.get_barrier_semaphore()

    def greet(target):
        pl.semaphore_signal(barrier, inc=1, device_id=target, device_id_type=MESH)

    cross = jnp.where(xl == 0, lax.rem(s + ns - 1, ns), lax.rem(s + 1, ns))
    cross_above = cross // 2 > z

    def in_column(k):
        to = along_z(k)
        return to, dev(2 * to + xl, r, m)

    for target in [partner, across, sides[0], sides[1]]:
        greet(target)

    @pl.loop(0, nmp - 1)
    def _(k):
        greet(dev(s, r, along_y(k)))

    @pl.loop(0, nz - 1)
    def _(k):
        to, target = in_column(k)

        @pl.when(to > z)
        def _():
            greet(target)

    @pl.when(cross_above)
    def _():
        greet(dev(cross, r, m))

    def enter():
        pl.semaphore_wait(barrier, 4 + (nmp - 1) + z + jnp.where(cross_above, 0, 1))

        @pl.loop(0, nz - 1)
        def _(k):
            to, target = in_column(k)

            @pl.when(to < z)
            def _():
                pl.semaphore_signal(above.at[z], inc=1, device_id=target, device_id_type=MESH)

        @pl.when(jnp.logical_not(cross_above))
        def _():
            pl.semaphore_signal(above_cross, inc=1, device_id=dev(cross, r, m), device_id_type=MESH)

    table.wait()

    wide = code.shape[1]
    lane = lax.broadcasted_iota(jnp.int32, (8, wide), 1)
    relay = lax.broadcasted_iota(jnp.int32, (8, wide), 0)
    value = jnp.full((8, wide), -1, jnp.int32)
    for j in range(2 * nz):
        chosen = jnp.where(relay == 0, tab[0, j] >> 20, tab[1, j] >> 20)
        value = jnp.where(lane // 8 == j, chosen * 8 + lane % 8, value)
    code[...] = value

    def compute(p, slots):
        live = lax.broadcasted_iota(jnp.int32, (rows, 128), 0) < (tab[p, 0] & 255)
        if slots:
            qs = {t: along_z(t) for t in slots}
            items = [(t, u) for t in slots for u in range(2)]
            x, back, wi, wo, pre, back_pre, act, grad, term = ({} for _ in range(9))
            for i in items:
                j = 2 * qs[i[0]] + i[1]
                x[i] = xs[p][:, pl.ds((tab[p, j] >> 20) * 128, 128)]
                wi[i] = wiv[p, j]
                pre[i] = contract(x[i], wi[i], 1, 0)
            for i in items:
                j = 2 * qs[i[0]] + i[1]
                picked = gs[p][:, pl.ds(((tab[p, j] >> 8) & 4095) * 128, 128)]
                back[i] = jnp.where(live, picked.astype(F32), 0.0).astype(BF16)
                wo[i] = wov[p, j]
                back_pre[i] = contract(back[i], wo[i], 1, 1)
            for i in items:
                v = pre[i]
                square = v * v
                th = jnp.tanh(ROOT * (v + CUBIC * (square * v)))
                half = 0.5 * (1.0 + th)
                act[i] = (v * half).astype(BF16)
                slope = half + (0.5 * v) * (1.0 - th * th) * (ROOT * (1.0 + (3.0 * CUBIC) * square))
                grad[i] = (back_pre[i] * slope).astype(BF16)
            for i in items:
                t, u = i
                outs = (contract(x[i], grad[i], 0, 0).astype(BF16), contract(act[i], back[i], 0, 0).astype(BF16))
                for kind in range(2):
                    for h in range(2):
                        for d in range(2):
                            lo = 32 * (2 * h + d)
                            part[p * groups + t // size, d, u, h, t % size, kind] = outs[kind][lo:lo + 32]
                term[i] = contract(grad[i], wi[i], 1, 1)
            for t in slots:
                at = pl.multiple_of(16 * qs[t], 16)
                for y in range(nmp):
                    both = jnp.concatenate([term[t, 0][8 * y:8 * y + 8], term[t, 1][8 * y:8 * y + 8]], axis=0)
                    terms[p, y, pl.ds(at, 16), :] = both.astype(BF16)

    def remote(src, dst, send, recv, target):
        return pltpu.make_async_remote_copy(
            src_ref=src, dst_ref=dst, send_sem=send, recv_sem=recv,
            device_id=target, device_id_type=MESH)

    def copy_a(n):
        return remote(part.at[n, 1 - c], from_core.at[n], a_send.at[n], a_recv.at[n], partner)

    def copies_b(n):
        out = [remote(pair.at[n, xl, 1 - xh], from_x.at[n, 0], b_send.at[n, 0], b_recv.at[n, 0], across)]
        for h in range(2):
            out.append(remote(pair.at[n, 1 - xl, h], from_x.at[n, 1 + xh],
                              b_send.at[n, 1 + h], b_recv.at[n, 1 + xh], sides[h]))
        return out

    def copy_c(n, t):
        p, g = n // groups, n % groups
        to = along_z(g * size + t)
        return remote(ready.at[n, t], landed.at[p, z], c_send.at[n, t], c_recv.at[p, z],
                      dev(2 * to + xl, r, m))

    def arrived_c(p, origin):
        return remote(landed.at[p, origin], landed.at[p, origin], c_send.at[0, 0], c_recv.at[p, origin], partner)

    def copy_t(p, to):
        return remote(terms.at[p, to], got.at[p, m], t_send.at[p, to], t_recv.at[p, m], dev(s, r, to))

    def arrived_t(p, origin):
        return remote(got.at[p, origin], got.at[p, origin], t_send.at[p, origin], t_recv.at[p, origin], partner)

    def copy_k(to):
        return remote(code, codes.at[m], k_send.at[to], k_recv.at[m], dev(s, r, to))

    def arrived_k(origin):
        return remote(codes.at[origin], codes.at[origin], k_send.at[origin], k_recv.at[origin], partner)

    cut = width // 2
    ends = jnp.logical_or(s == 0, s == ns - 1)
    beside = jnp.logical_or(s == 1, s == ns - 2)

    def outward(p):
        return jnp.logical_not(jnp.logical_and(ends, xl == p))

    def inward(p):
        return jnp.logical_not(jnp.logical_and(ends, xl == 1 - p))
    back_turn = jnp.where(xl == 0, 2, ns - 2)
    side = dev(2 * z + (1 - xl), r, m)
    along = dev(lax.rem(s + back_turn, ns), r, m)

    def copy_d(p):
        return remote(dx.at[p, :, :cut], dx_in.at[p, :, :cut], d_send.at[p], d_recv.at[p], (down, up)[p])

    def copy_e():
        return remote(dx.at[1 - xl, :, cut:], dx_in.at[1 - xl, :, cut:], e_send, e_recv.at[1 - xl], side)

    def copy_hop():
        return remote(dx.at[xl, :, cut:], hop, h_send.at[0], h_recv, side)

    def forward():
        return remote(hop, dx_in.at[1 - xl, :, cut:], h_send.at[1], e_recv.at[1 - xl], along)

    def arrived_e(p):
        return remote(dx_in.at[p, :, cut:], dx_in.at[p, :, cut:], e_send, e_recv.at[p], partner)

    def send_terms(p):
        @pl.loop(0, nmp - 1)
        def _(k):
            copy_t(p, along_y(k)).start()
        got[p, m] = terms[p, m]

    def add_pair(n):
        copy_a(n).wait_recv()
        copies = copies_b(n)
        for u in range(2):
            for h in range(2):
                pair[n, u, h] = part[n, c, u, h] + from_core[n, u, h]
        for copy in copies:
            copy.start()

    def add_x(n):
        for i in range(3):
            remote(from_x.at[n, i], from_x.at[n, i], b_send.at[n, i], b_recv.at[n, i], across).wait_recv()
        g = n % groups
        last = size - 1 if g == groups - 1 else size
        for t in range(size):
            ready[n, t, xl] = pair[n, xl, xh, t] + from_x[n, 0, t]
            ready[n, t, 1 - xl] = from_x[n, 1, t] + from_x[n, 2, t]
            if t < last:
                if n < groups:
                    to = along_z(g * size + t)

                    @pl.when(to > z)
                    def _():
                        pl.semaphore_wait(above.at[to], 1)
                copy_c(n, t).start()
        if g == groups - 1:
            landed[n // groups, z] = ready[n, size - 1]

    def scatter(p):
        first = pl.multiple_of(16 * (m // 2), 16)
        odd = lax.rem(m, 2) == 1
        row = lax.broadcasted_iota(jnp.int32, (8, 128), 0) + 8 * m
        span = 8 * ns
        tile = 8 * count // 3 if (8 * count) % 96 == 0 else 8 * count

        @pl.loop(0, nmp - 1)
        def _(i):
            arrived_t(p, along_y(i)).wait_recv()

        @pl.loop(0, 8 * count // tile)
        def _(i):
            base = i * tile
            place = lax.broadcasted_iota(jnp.int32, (tile, span), 0) + base
            total = jnp.zeros((tile, 128), F32)
            for y in range(nmp):
                hot = (place == codes[y, p:p + 1, :span]).astype(F32).astype(BF16)
                total = total + contract(hot, got[p, y], 1, 0)
            for b in range(tile // 8):
                at = pl.multiple_of(base * 16 + b * 128, 128)
                mine = gs[p][pl.ds(first, 16), pl.ds(at, 128)].astype(F32)
                mine = jnp.where(odd, mine[8:16], mine[0:8])
                mine = jnp.where(row < (tab[p, 0] & 255), mine, 0.0)
                dx[p, :, pl.ds(at, 128)] = (mine + total[8 * b:8 * b + 8]).astype(BF16)

        @pl.when(outward(p))
        def _():
            copy_d(p).start()

    steps = [(p, list(range(t, min(t + PER, nz)))) for p in range(2) for t in range(0, nz, PER)]
    half = len(steps) // 2
    early = 1

    def chunks_of(step):
        p, slots = step
        return sorted({p * groups + t // size for t in slots})

    for load in loads[0]:
        load.wait()
    for load in loads[1]:
        load.start()
    for step in steps[:early]:
        compute(*step)
    enter()
    for step in steps[:early]:
        for n in chunks_of(step):
            copy_a(n).start()

    @pl.loop(0, nmp - 1)
    def _(k):
        copy_k(along_y(k)).start()
    codes[m] = code[...]
    if early == half:
        send_terms(0)
    paired = moved = 0
    for i in range(early, len(steps)):
        if i == half:
            for load in loads[1]:
                load.wait()
        if HEAD and i == len(steps) - 1 and i > half:
            for _ in range(HEAD):
                add_x(moved)
                moved += 1
        compute(*steps[i])
        for n in chunks_of(steps[i]):
            copy_a(n).start()
        if i == half - 1:
            send_terms(0)
        while paired <= chunks_of(steps[i - 1])[-1]:
            add_pair(paired)
            paired += 1
    send_terms(1)
    lead = moved + 1
    while moved < chunks:
        if paired < chunks and moved >= lead:
            add_pair(paired)
            paired += 1
        add_x(moved)
        moved += 1

    @pl.loop(0, nmp - 1)
    def _(i):
        arrived_k(along_y(i)).wait_recv()
    @pl.when(cross_above)
    def _():
        pl.semaphore_wait(above_cross, 1)
    for p in range(2):
        scatter(p)
    copy_e().start()

    @pl.when(jnp.logical_not(ends))
    def _():
        copy_hop().start()

    @pl.when(jnp.logical_not(beside))
    def _():
        copy_hop().wait_recv()
        forward().start()

    for n in range(chunks):
        copy_a(n).wait_send()
        for copy in copies_b(n):
            copy.wait_send()

    @pl.loop(0, nmp - 1)
    def _(i):
        copy_k(along_y(i)).wait_send()
        for p in range(2):
            copy_t(p, along_y(i)).wait_send()

    def take(p):
        @pl.when(inward(p))
        def _():
            copy_d(p).wait_recv()
            arrived_e(p).wait_recv()
            passed_ref[p] = dx_in[p]

        @pl.when(jnp.logical_not(inward(p)))
        def _():
            passed_ref[p] = jnp.zeros(passed_ref.shape[1:], BF16)

    def total(o):
        q = nz - 1 - o
        for u in range(2):
            for kind in range(2):
                grads_ref[2 * q + u, kind] = (landed[0, q, u, kind].astype(F32)
                                              + landed[1, o, 1 - u, kind].astype(F32))

    @pl.loop(0, nz - 1)
    def _(k):
        arrived_c(0, along_z(k)).wait_recv()
    total(z)
    take(0)

    @pl.loop(0, nz - 1)
    def _(k):
        o = along_z(k)
        arrived_c(1, o).wait_recv()
        total(o)
    take(1)

    for n in range(chunks):
        last = size - 1 if n % groups == groups - 1 else size

        @pl.loop(0, last)
        def _(t):
            copy_c(n, t).wait_send()
    for p in range(2):
        @pl.when(outward(p))
        def _():
            copy_d(p).wait_send()
    copy_e().wait_send()

    @pl.when(jnp.logical_not(ends))
    def _():
        copy_hop().wait_send()

    @pl.when(jnp.logical_not(beside))
    def _():
        forward().wait_send()


def body(section_in, out_grad, lengths, w_in, w_out, idx_in, idx_out):
    x = section_in[:, 0]
    g = out_grad[:, 0]
    rows, width = x.shape[1:]
    nf = w_in.shape[2]
    nz = lax.axis_size("section") // 2
    nmp = lax.axis_size("mp")
    wide = -(-8 * nf // 128) * 128
    groups = 6 if nz % 6 == 0 else 1
    chunks, size = 2 * groups, nz // groups
    dma = pltpu.SemaphoreType.DMA
    hbm = pl.BlockSpec(memory_space=pltpu.HBM)
    vmem = pl.BlockSpec(memory_space=pltpu.VMEM)
    slab = (size, 2, 32, 128)
    table = (idx_in[0] * 4096 + idx_out[0]) * 256 + lengths[:, 0]
    passed, grads = pl.pallas_call(
        functools.partial(kernel, nz, nmp, groups),
        out_shape=(
            jax.ShapeDtypeStruct((2, 8, width), BF16),
            jax.ShapeDtypeStruct((nf, 2, 32, 128), F32),
        ),
        in_specs=[hbm] * 5,
        out_specs=(vmem, vmem),
        scratch_shapes=[
            pltpu.SMEM((2, nf), jnp.int32),
            pltpu.VMEM((rows, width), BF16),
            pltpu.VMEM((rows, width), BF16),
            pltpu.VMEM((rows, width), BF16),
            pltpu.VMEM((rows, width), BF16),
            pltpu.VMEM((2, nf, 128, 128), BF16),
            pltpu.VMEM((2, nf, 128, 128), BF16),
            pltpu.VMEM((chunks, 2, 2, 2) + slab, BF16),
            pltpu.VMEM((chunks, 2, 2) + slab, BF16),
            pltpu.VMEM((chunks, 2, 2) + slab, BF16),
            pltpu.VMEM((chunks, 3) + slab, BF16),
            pltpu.VMEM((chunks, size, 2, 2, 32, 128), BF16),
            pltpu.VMEM((2, nz, 2, 2, 32, 128), BF16),
            pltpu.VMEM((2, nmp, 8 * nf, 128), BF16),
            pltpu.VMEM((2, nmp, 8 * nf, 128), BF16),
            pltpu.VMEM((8, wide), jnp.int32),
            pltpu.VMEM((nmp, 8, wide), jnp.int32),
            pltpu.VMEM((2, 8, width), BF16),
            pltpu.VMEM((2, 8, width), BF16),
            pltpu.VMEM((8, width // 2), BF16),
            dma((2, 4)), dma, dma((chunks,)), dma((chunks,)), dma((chunks, 3)), dma((chunks, 3)),
            dma((chunks, size)), dma((2, nz)), dma((2, nmp)), dma((2, nmp)),
            dma((nmp,)), dma((nmp,)), dma((2,)), dma((2,)), dma, dma((2,)), dma((2,)), dma,
            pltpu.SemaphoreType.REGULAR((nz,)), pltpu.SemaphoreType.REGULAR,
        ],
        compiler_params=pltpu.CompilerParams(
            collective_id=0, has_side_effects=True, vmem_limit_bytes=52 * 2**20),
    )(table, x, g, w_in[0], w_out[0])
    return passed[:, None], grads[:, :, None, None]


def solution(mesh):
    placed = (
        P(None, "section", "dp", None),
        P(None, "section", "dp", None),
        P(None, "section", "dp"),
        P("section", None, "mp", None, None),
        P("section", None, "mp", None, None),
        P("section", None, "mp"),
        P("section", None, "mp"),
    )
    return jax.shard_map(
        body,
        mesh=mesh,
        in_specs=placed,
        out_specs=(
            P(None, "section", ("dp", "mp"), None),
            P(None, None, "mp", "section", "dp", None),
        ),
        check_vma=False,
    )
```
